32 devices in a mesh: geo: 4 (over x, core), comp: 8 (over z, y).
Axes of the slice: x: 2, y: 2, z: 4, core: 2. Of those that a mesh axis runs over, the one named last changes fastest.
Arguments:
- spectrum: bfloat16 [1152, 512, 128], P('comp', 'geo'), may hold values from 0.049804688 to 1
- land_mask: int32 [512, 128], P('geo'), may hold values 0 or 1
- wind_speed: float32 [512, 128], P('geo'), may hold values from 0.5 to 2
- wind_dir: float32 [512, 128], P('geo'), may hold values from -3.140625 to 3.140625
- input_rate: float32 [1152], P('comp'), may hold values from 0.05 to 0.5
- dissipation: float32 [1152], replicated, may hold values from 0.05 to 0.5
- pair_first: bfloat16 [1728, 1152], replicated, may hold values from -0.1875 to 0.1875
- pair_second: bfloat16 [1728, 1152], replicated, may hold values from -0.1875 to 0.1875
- merge_weight: bfloat16 [1152, 1728], replicated, may hold values from -0.15625 to 0.15625
Outputs:
- spectrum_next: bfloat16 [1152, 512, 128], P('comp', 'geo')
The draws below stay inside these ranges and needn't reach their ends.
All inputs are finite; a program needn't handle non-finite values. No bound on the sum of `land_mask` on one device may be relied on, other than what follows from the above.
Results may differ from the reference program's by a relative error of at most 0.0038.
Values may be sent and summed in bfloat16 or wider, within the bound.
A program may use at most 128 MiB of HBM per device.

```python
import math
import jax
import jax.numpy as jnp
from jax import lax

NF = 32
ND = 36
M = 1152
Q = 1728
X = 128
PROP_STEPS = 6
NY = 512


def place_ends(drawn, own_key, smallest, high):
    shape = drawn.shape
    index_at = [jax.random.randint(jax.random.fold_in(own_key, axis), (), 0, shape[axis]) for axis in range(len(shape))]
    drawn = drawn.at[tuple(index_at)].set(smallest)
    longest = shape.index(max(shape))
    index_at[longest] = (index_at[longest] + 1) % shape[longest]
    return drawn.at[tuple(index_at)].set(high)


def block_levels(key, shape, pieces, smallest, top_value):
    factor_of = 1.0
    for axis_at, blocks in pieces:
        draws = jax.random.uniform(jax.random.fold_in(jax.random.fold_in(key, 6), axis_at), (blocks,), jnp.float32, smallest / len(pieces), top_value / len(pieces))
        factor_of = factor_of * jnp.repeat(jnp.exp(draws), shape[axis_at] // blocks).reshape((-1,) + (1,) * (len(shape) - 1 - axis_at))
    return factor_of


def bell_draw(rng, shape, width, limit, kind=jnp.bfloat16):
    return jnp.clip(width * jax.random.normal(rng, shape, jnp.float32), -limit, limit).astype(kind)


def setup_inputs(seed: int = 0) -> dict:
    arg_keys = jax.random.split(jax.random.key(seed), 10)
    return {
        "spectrum": jnp.clip(jnp.exp(math.log(1.0) - 2.9996462 * jax.random.uniform(arg_keys[0], (M, NY, X), jnp.float32) ** block_levels(arg_keys[0], (M, NY, X), ((0, 8), (1, 4)), -0.2, 0.2)), 0.049804688, 1.0).astype(jnp.bfloat16),
        "land_mask": place_ends((jax.random.randint(arg_keys[1], (NY, X), 0, 4) < 3).astype(jnp.int32), jax.random.fold_in(arg_keys[1], 1), 0, 1),
        "wind_speed": jnp.clip(jnp.exp(math.log(2.0) - 1.3862944 * jax.random.uniform(arg_keys[2], (NY, X), jnp.float32) ** block_levels(arg_keys[2], (NY, X), ((0, 4),), -0.2, 0.2)), 0.5, 2.0),
        "wind_dir": jnp.clip(jax.random.uniform(arg_keys[3], (NY, X), jnp.float32, -3.140625, 3.140625), -3.140625, 3.140625),
        "input_rate": jnp.clip(jnp.exp(math.log(0.5) - 2.3025851 * jax.random.uniform(arg_keys[4], (M,), jnp.float32) ** block_levels(arg_keys[4], (M,), ((0, 8),), -0.2, 0.2)), 0.05, 0.5),
        "dissipation": jnp.clip(jnp.exp(jax.random.uniform(arg_keys[5], (M,), jnp.float32, math.log(0.05), math.log(0.5))), 0.05, 0.5),
        "pair_first": bell_draw(arg_keys[6], (Q, M), M ** -0.5, 0.1875),
        "pair_second": bell_draw(arg_keys[7], (Q, M), M ** -0.5, 0.1875),
        "merge_weight": bell_draw(arg_keys[8], (M, Q), Q ** -0.5, 0.15625),
    }


def upwind(padded, sea_mask, speed_x, speed_y):
    center = padded[:, 1:-1]
    lower = padded[:, :-2]
    upper = padded[:, 2:]
    western = jnp.roll(center, 1, axis=2)
    eastern = jnp.roll(center, -1, axis=2)
    change = jnp.maximum(speed_x, 0.0) * (center - western) + jnp.maximum(-speed_x, 0.0) * (center - eastern)
    change = change + jnp.maximum(speed_y, 0.0) * (center - lower) + jnp.maximum(-speed_y, 0.0) * (center - upper)
    return (center - change) * sea_mask

def speeds(comp_ids):
    frequency = (comp_ids // ND).astype(jnp.float32)
    heading = 2.0 * math.pi * (comp_ids % ND).astype(jnp.float32) / ND
    courant = 0.7 * jnp.power(jnp.float32(1.1), -frequency)
    speed_x = (courant * jnp.cos(heading))[:, None, None]
    speed_y = (courant * jnp.sin(heading))[:, None, None]
    return (heading, speed_x, speed_y)

def propagate(density, sea_mask, substeps):
    blocks = density.reshape(NF, ND, NY, X)

    def along(args):
        block, freq_index = args
        comp_ids = freq_index * ND + jnp.arange(ND, dtype=jnp.int32)
        heading, speed_x, speed_y = speeds(comp_ids)
        for repeat in range(substeps):
            padded = jnp.pad(block, ((0, 0), (1, 1), (0, 0)))
            block = upwind(padded, sea_mask, speed_x, speed_y)
        return block
    return lax.map(along, (blocks, jnp.arange(NF, dtype=jnp.int32))).reshape(M, NY, X)

def point_sources(spectra, dissipation, pair_first, pair_second, merge_weight):
    values = spectra.astype(jnp.float32)
    first_proj = jnp.dot(pair_first.astype(jnp.float32), values, precision=lax.Precision.HIGHEST)
    second_proj = jnp.dot(pair_second.astype(jnp.float32), values, precision=lax.Precision.HIGHEST)
    product = (first_proj * second_proj).astype(jnp.bfloat16)
    transfer = jnp.dot(merge_weight.astype(jnp.float32), product.astype(jnp.float32), precision=lax.Precision.HIGHEST)
    energy = lax.optimization_barrier(jnp.sum(values, axis=0))
    whitecap = -dissipation[:, None] * jnp.sqrt(energy / M + 1e-06)[None, :] * values
    return (transfer + whitecap).astype(jnp.bfloat16)

def reference(spectrum, land_mask, wind_speed, wind_dir, input_rate, dissipation, pair_first, pair_second, merge_weight):
    sea_mask = land_mask.astype(jnp.float32)
    density = propagate(spectrum.astype(jnp.float32), sea_mask, PROP_STEPS)
    outgoing = density.astype(jnp.bfloat16)
    groups = NY // 8
    stacked = outgoing.reshape(M, groups, 8 * X).transpose(1, 0, 2)
    increment = lax.map(lambda spectra: point_sources(spectra, dissipation, pair_first, pair_second, merge_weight), stacked)
    increment = increment.transpose(1, 0, 2).reshape(M, NY, X)
    heading, speed_x, speed_y = speeds(jnp.arange(M, dtype=jnp.int32))
    facing = jnp.maximum(jnp.cos(heading[:, None, None] - wind_dir[None]), 0.0)
    growth = input_rate[:, None, None] * wind_speed[None] * facing * facing
    density = density + growth * density + increment.astype(jnp.float32)
    density = propagate(density, sea_mask, 1)
    return density.astype(jnp.bfloat16)
```

```python
import functools
import math

import jax
import jax.numpy as jnp
from jax import lax
from jax.experimental import pallas as pl
from jax.experimental.pallas import tpu as pltpu
from jax.sharding import PartitionSpec as P

ND = 36
PROP_STEPS = 6
HALO = 8
SENDS = 3
RETURNS = 2
F32 = jnp.float32
BF16 = jnp.bfloat16
VMEM = pltpu.VMEM
SMEM = pltpu.SMEM


def edges(cells, axis_dim):
    count = lax.axis_size("geo")
    ends = count - 1
    size = cells.shape[axis_dim]
    head = lax.slice_in_dim(cells, 0, HALO, axis=axis_dim)
    tail = lax.slice_in_dim(cells, size - HALO, size, axis=axis_dim)
    lower = lax.ppermute(tail, "geo", [(i, i + 1) for i in range(ends)])
    upper = lax.ppermute(head, "geo", [(i + 1, i) for i in range(ends)])
    return lower, upper


def block_of(comps):
    return 16 if comps % 16 == 0 else comps


def stride_of(block):
    return -(-block // 8) * 8


def upwind(v, mask, coef, at):
    center, west, east, south, north = (coef[at + k] for k in range(5))
    rows = v.shape[0]
    moved = west * pltpu.roll(v, 1, 1) + east * pltpu.roll(v, v.shape[1] - 1, 1)
    moved = moved + south * pltpu.roll(v, 1, 0) + north * pltpu.roll(v, rows - 1, 0)
    return (center * v + moved) * mask


def prop_kernel(coef, lower, cells, upper, mask, density, outgoing, turned):
    block, rows, cols = cells.shape
    stride = stride_of(block)
    first = pl.program_id(0) * block

    def one(c, carry):
        v = jnp.concatenate(
            [lower[c].astype(F32), cells[c].astype(F32), upper[c].astype(F32)], axis=0
        )
        sea = mask[...]
        for _ in range(PROP_STEPS):
            v = upwind(v, sea, coef, (first + c) * 8)
        density[c] = v
        turned[pl.ds(c, rows, stride=stride), :] = v[HALO : HALO + rows]
        return carry

    lax.fori_loop(0, block, one, 0)

    def pack(r, carry):
        start = pl.multiple_of(r * stride, 8)
        outgoing[r] = turned[pl.ds(start, block), :].astype(BF16)
        return carry

    lax.fori_loop(0, rows, pack, 0, unroll=8)


def propagate(coef, lower, cells, upper, mask):
    comps, rows, cols = cells.shape
    block = block_of(comps)
    tall = rows + 2 * HALO
    return pl.pallas_call(
        prop_kernel,
        grid=(comps // block,),
        in_specs=[
            pl.BlockSpec(memory_space=SMEM),
            pl.BlockSpec((block, HALO, cols), lambda i: (i, 0, 0)),
            pl.BlockSpec((block, rows, cols), lambda i: (i, 0, 0)),
            pl.BlockSpec((block, HALO, cols), lambda i: (i, 0, 0)),
            pl.BlockSpec((tall, cols), lambda i: (0, 0)),
        ],
        out_specs=[
            pl.BlockSpec((block, tall, cols), lambda i: (i, 0, 0)),
            pl.BlockSpec((rows, block, cols), lambda i: (0, i, 0)),
        ],
        out_shape=[
            jax.ShapeDtypeStruct((comps, tall, cols), F32),
            jax.ShapeDtypeStruct((rows, comps, cols), BF16),
        ],
        scratch_shapes=[VMEM((rows * stride_of(block), cols), F32)],
        cost_estimate=pl.CostEstimate(
            flops=comps * tall * cols * 100,
            bytes_accessed=comps * tall * cols * 8,
            transcendentals=0,
        ),
        name="propagate",
    )(coef, lower, cells, upper, mask)


def point_kernel(sends, *refs):
    near, far = refs[:sends], refs[sends : 2 * sends]
    loss, first, second, merge, out, spectra, product = refs[2 * sends :]
    peers, _, part, cols = near[0].shape
    local = sends * part
    comps, terms = merge.shape
    for side, group in enumerate((near, far)):
        lanes = slice(side * cols, (side + 1) * cols)
        for k in range(sends):
            for s in range(peers):
                at = s * local + k * part
                spectra[at : at + part, lanes] = group[k][s, 0]
    tile = max(t for t in range(16, 600, 16) if terms % t == 0)

    def multiply(t, carry):
        rows = pl.ds(pl.multiple_of(t * tile, 16), tile)
        x = spectra[...]
        one = jnp.dot(first[rows, :], x, preferred_element_type=F32)
        two = jnp.dot(second[rows, :], x, preferred_element_type=F32)
        product[rows, :] = (one * two).astype(BF16)
        return carry

    lax.fori_loop(0, terms // tile, multiply, 0)
    energy = jnp.sum(spectra[...].astype(F32), axis=0, keepdims=True)
    root = jnp.sqrt(energy / comps + 1e-06)
    if peers == 1:
        step = max(t for t in range(16, 600, 16) if comps % t == 0)
        for d in range(0, comps, step):
            rows = slice(d, d + step)
            moved = jnp.dot(merge[rows, :], product[...], preferred_element_type=F32)
            total = moved - loss[rows, :] * root * spectra[rows, :].astype(F32)
            out[0, 0, rows] = total[:, :cols].astype(BF16)
            out[0, 1, rows] = total[:, cols:].astype(BF16)
        return
    share = max(g for g in range(1, peers + 1) if peers % g == 0 and g * local <= 600)
    for d in range(0, peers, share):
        rows = slice(d * local, (d + share) * local)
        moved = jnp.dot(merge[rows, :], product[...], preferred_element_type=F32)
        total = moved - loss[rows, :] * root * spectra[rows, :].astype(F32)
        for g in range(share):
            piece = total[g * local : (g + 1) * local].astype(BF16)
            out[d + g, 0] = piece[:, :cols]
            out[d + g, 1] = piece[:, cols:]


def point_terms(chunks, start, pairs, loss, first, second, merge):
    sends = len(chunks)
    peers, rows, part, cols = chunks[0].shape
    local = sends * part
    comps, terms = merge.shape
    whole = lambda shape: pl.BlockSpec(shape, lambda i: (0, 0))
    near = pl.BlockSpec((peers, 1, part, cols), lambda i: (0, start + i, 0, 0))
    far = pl.BlockSpec((peers, 1, part, cols), lambda i: (0, rows - 1 - start - i, 0, 0))
    return pl.pallas_call(
        functools.partial(point_kernel, sends),
        grid=(pairs,),
        in_specs=[near] * sends
        + [far] * sends
        + [whole((comps, 1)), whole((terms, comps)), whole((terms, comps)), whole((comps, terms))],
        out_specs=pl.BlockSpec((peers, 2, local, cols), lambda i: (0, i, 0, 0)),
        out_shape=jax.ShapeDtypeStruct((peers, 2 * pairs, local, cols), BF16),
        scratch_shapes=[VMEM((comps, 2 * cols), BF16), VMEM((terms, 2 * cols), BF16)],
        cost_estimate=pl.CostEstimate(
            flops=pairs * 12 * comps * terms * cols,
            bytes_accessed=6 * comps * terms + pairs * 8 * comps * cols,
            transcendentals=0,
        ),
        compiler_params=pltpu.CompilerParams(vmem_limit_bytes=60 * 1024 * 1024),
        name="points",
    )(*chunks, *chunks, loss, first, second, merge)


def final_kernel(returns, coef, density, low_inc, high_inc, wind, mask, *refs):
    incs = refs[:returns]
    out, turned = refs[returns:]
    block, rows, cols = out.shape
    peers, held = incs[0].shape[:2]
    band = rows // peers
    stride = stride_of(block)
    first = pl.program_id(0) * block

    def place(s, carry):
        for k in range(returns):
            for j in range(held):
                a = k * (held // 2) + j // 2
                row = a if j % 2 == 0 else band - 1 - a
                at = pl.multiple_of((s * band + row) * stride, 8)
                turned[pl.ds(at, block), :] = incs[k][s, j].astype(F32)
        return carry

    lax.fori_loop(0, peers, place, 0)

    def one(c, carry):
        at = (first + c) * 8
        inc = jnp.concatenate(
            [low_inc[c], turned[pl.ds(c, rows, stride=stride), :], high_inc[c]], axis=0
        )
        v = density[c]
        facing = jnp.maximum(coef[at + 6] * wind[1] + coef[at + 7] * wind[2], 0.0)
        growth = coef[at + 5] * wind[0] * facing * facing
        v = v + growth * v + inc
        v = upwind(v, mask[...], coef, at)
        out[c] = v[HALO : HALO + rows].astype(BF16)
        return carry

    lax.fori_loop(0, block, one, 0)


def finish(coef, density, low_inc, high_inc, wind, mask, incs, lead):
    local, tall, cols = density.shape
    rows = tall - 2 * HALO
    block = block_of(local)
    peers, held = incs[0].shape[:2]
    return pl.pallas_call(
        functools.partial(final_kernel, len(incs)),
        grid=(local // block,),
        in_specs=[
            pl.BlockSpec(memory_space=SMEM),
            pl.BlockSpec((block, tall, cols), lambda i: (i, 0, 0)),
            pl.BlockSpec((block, HALO, cols), lambda i: (i, 0, 0)),
            pl.BlockSpec((block, HALO, cols), lambda i: (i, 0, 0)),
            pl.BlockSpec((3, tall, cols), lambda i: (0, 0, 0)),
            pl.BlockSpec((tall, cols), lambda i: (0, 0)),
        ]
        + [pl.BlockSpec((peers, held, block, cols), lambda i: (0, 0, i, 0))] * len(incs),
        out_specs=pl.BlockSpec((block, rows, cols), lambda i: (i, 0, 0)),
        out_shape=jax.ShapeDtypeStruct((local, rows, cols), BF16),
        scratch_shapes=[VMEM((rows * stride_of(block), cols), F32)],
        name="finish",
    )(coef, density, low_inc, high_inc, wind, mask, *incs)


def body(spectrum, land_mask, wind_speed, wind_dir, input_rate, dissipation, pair_first, pair_second, merge_weight):
    local, rows, cols = spectrum.shape
    peers = lax.axis_size("comp")
    band = rows // peers
    ids = lax.axis_index("comp") * local + jnp.arange(local, dtype=jnp.int32)
    frequency = (ids // ND).astype(F32)
    heading = 2.0 * math.pi * (ids % ND).astype(F32) / ND
    courant = 0.7 * jnp.power(F32(1.1), -frequency)
    cos_h, sin_h = jnp.cos(heading), jnp.sin(heading)
    west, east = jnp.maximum(courant * cos_h, 0.0), jnp.maximum(-courant * cos_h, 0.0)
    south, north = jnp.maximum(courant * sin_h, 0.0), jnp.maximum(-courant * sin_h, 0.0)
    center = 1.0 - west - east - south - north
    coef = jnp.stack([center, west, east, south, north, input_rate, cos_h, sin_h], axis=1).reshape(-1)

    lower, upper = edges(spectrum, 1)
    fields = jnp.stack([wind_speed, jnp.cos(wind_dir), jnp.sin(wind_dir), land_mask.astype(F32)])
    low_f, high_f = edges(fields, 1)
    fields = jnp.concatenate([low_f, fields, high_f], axis=1)
    wind, mask = fields[:3], fields[3]

    whole_tiles = local % (16 * SENDS) == 0
    sends = SENDS if whole_tiles else 1
    part = local // sends
    density, chunks = [], []
    for k in range(sends):
        cut = slice(k * part, (k + 1) * part)
        d, out = propagate(coef[k * part * 8 : (k + 1) * part * 8], lower[cut], spectrum[cut], upper[cut], mask)
        density.append(d)
        out = out.reshape(peers, band, part, cols)
        chunks.append(lax.all_to_all(out, "comp", split_axis=0, concat_axis=0, tiled=True))
    density = jnp.concatenate(density, axis=0)

    loss = dissipation[:, None]
    if not whole_tiles:
        chunks = [c.transpose(1, 0, 2, 3).reshape(1, band, peers * local, cols) for c in chunks]
    returns = max(1, min(RETURNS, band // 2))
    pairs = band // 2 // returns
    incs = []
    for k in range(returns):
        inc = point_terms(chunks, k * pairs, pairs, loss, pair_first, pair_second, merge_weight)
        if not whole_tiles:
            inc = inc.reshape(2 * pairs, peers, local, cols).transpose(1, 0, 2, 3)
        incs.append(lax.all_to_all(inc, "comp", split_axis=0, concat_axis=0, tiled=True))
    count = lax.axis_size("geo")
    ends = count - 1
    low = lax.ppermute(incs[0][peers - 1, 1], "geo", [(i, i + 1) for i in range(ends)])
    high = lax.ppermute(incs[0][0, 0], "geo", [(i + 1, i) for i in range(ends)])
    low = jnp.pad(low.astype(F32)[:, None], ((0, 0), (HALO - 1, 0), (0, 0)))
    high = jnp.pad(high.astype(F32)[:, None], ((0, 0), (0, HALO - 1), (0, 0)))
    return finish(coef, density, low, high, wind, mask, incs, HALO)


def solution(mesh):
    placed = (P("comp", "geo", None), P("geo", None), P("geo", None), P("geo", None), P("comp"), P(), P(), P(), P())
    return jax.shard_map(
        body, mesh=mesh, in_specs=placed, out_specs=P("comp", "geo", None), check_vma=False
    )
```
